32 devices in a mesh: dom: 32 (over z, y, x, core).
Axes of the slice: x: 2, y: 2, z: 4, core: 2. Of those that a mesh axis runs over, the one named last changes fastest.
Arguments:
- tracers: float32 [20, 8, 32768], P(None, None, 'dom'), may hold values from -6 to 6
- mass_flux: float32 [3, 8, 32768], P(None, None, 'dom'), may hold values from -6 to 6
- lsq_coeff: float32 [2, 3, 32768], P(None, None, 'dom'), may hold values from -3 to 3
- own_offset: float32 [2, 3, 8, 32768], P(None, None, None, 'dom'), may hold values from -1.5 to 1.5
- far_offset: float32 [2, 3, 8, 32768], P(None, None, None, 'dom'), may hold values from -1.5 to 1.5
- inv_mass: float32 [8, 32768], P(None, 'dom'), may hold values from 0.25 to 1
- neighbour: int32 [3, 32768], P(None, 'dom'), may hold values from 0 to 1791, as said below
- send_cells: int32 [6, 4096], P(None, 'dom'), may hold values from 0 to 1023, as said below
Outputs:
- updated: float32 [20, 8, 32768], P(None, None, 'dom')
The draws below stay inside these ranges and needn't reach their ends.
Inputs may be any that keep to these rules, and one draw needn't show every extreme that they name: For each domain, entries index its 1024 own cells followed by 6 received blocks of 128 slots; every referenced received slot holds a real cell of the sending domain, the unused tail of a block is never referenced, and for every neighbour slot some domain references a block in full. `send_cells`: each block of 128 entries (one sending domain, one neighbour slot) lists distinct own cells of the sending domain, as local indices.
All inputs are finite; a program needn't handle non-finite values.
Results may differ from the reference program's by a relative error of at most 0.0003.
Values sent between devices are 32-bit elements; how exact they have to be, the bound alone decides.
A program may use at most 64 MiB of HBM per device.

```python
import math
import jax
import jax.numpy as jnp

TRC = 20
LEV = 8
CEL_DEV = 1024
PEERS = 6
HALO = 128
NCELL = 32768


def peer_shift_drawn(peer_slot):
    return (peer_slot // 2 + 1) * (1 - 2 * (peer_slot % 2))


def mesh_tables(key):
    devices = NCELL // CEL_DEV
    offsets = jnp.array([peer_shift_drawn(peer_slot) for peer_slot in range(PEERS)], jnp.int32)
    fewest = max(1, HALO // 4)
    counts = jax.random.randint(jax.random.fold_in(key, 101), (devices, PEERS), fewest, HALO + 1)
    full_rank = jax.random.randint(jax.random.fold_in(key, 102), (PEERS,), 0, devices)
    counts = jnp.where(jnp.arange(devices)[:, None] == full_rank[None, :], HALO, counts)
    send_keys = jax.random.split(jax.random.fold_in(key, 103), devices * PEERS)

    def pick_cells(subkey):
        return jax.random.permutation(subkey, CEL_DEV)[:HALO]
    chosen = jax.vmap(pick_cells)(send_keys)
    send_table = chosen.reshape(devices, PEERS, HALO).transpose(1, 0, 2).reshape(PEERS, devices * HALO)
    sender = (jnp.arange(devices)[:, None] - offsets[None, :]) % devices
    recv_counts = counts[sender, jnp.arange(PEERS)[None, :]]
    slot_range = jnp.arange(HALO)
    usable = slot_range[None, None, :] < recv_counts[:, :, None]
    values = CEL_DEV + jnp.arange(PEERS)[:, None] * HALO + slot_range[None, :]
    slot_table = jnp.where(usable, values[None], -1).reshape(devices, PEERS * HALO)
    filler = jnp.full((devices, 3 * CEL_DEV - PEERS * HALO), -1, slot_table.dtype)
    padded = jnp.concatenate([slot_table, filler], axis=1)
    place_keys = jax.random.split(jax.random.fold_in(key, 104), devices)

    def place_row(subkey, slot_row):
        return slot_row[jax.random.permutation(subkey, 3 * CEL_DEV)]
    placed = jax.vmap(place_row)(place_keys, padded).reshape(devices, 3, CEL_DEV)
    jumps = jax.random.randint(jax.random.fold_in(key, 105), (devices, 3, CEL_DEV), 1, CEL_DEV)
    local_pick = (jnp.arange(CEL_DEV)[None, None, :] + jumps) % CEL_DEV
    neighbour_table = jnp.where(placed >= 0, placed, local_pick).transpose(1, 0, 2).reshape(3, devices * CEL_DEV)
    return (neighbour_table.astype(jnp.int32), send_table.astype(jnp.int32))


def draw_neighbour(key, part):
    return mesh_tables(key)[0]


def draw_send_cells(key, part):
    return mesh_tables(key)[1]


def steps_of(own_key, extent, cuts, low, high):
    def one(position, blocks):
        draws = jax.random.uniform(jax.random.fold_in(jax.random.fold_in(own_key, 6), position), (blocks,), jnp.float32, low / len(cuts), high / len(cuts))
        return jnp.repeat(jnp.exp(draws), extent[position] // blocks).reshape((-1,) + (1,) * (len(extent) - position - 1))

    level = one(*cuts[0])
    for cut in cuts[1:]:
        level = level * one(*cut)
    return level


def noise(rng, dims, width, reach, cuts=(), held_as=jnp.bfloat16):
    result = width * jax.random.normal(rng, dims, jnp.float32)
    if cuts:
        result = result * steps_of(rng, dims, cuts, -0.22, 0.18)
    return jnp.clip(result, -reach, reach).astype(held_as)


def setup_inputs(seed: int = 0) -> dict:
    arg_keys = jax.random.split(jax.random.key(seed), 9)
    tracers = noise(arg_keys[0], (TRC, LEV, NCELL), 1.0, 6.0, ((2, 32),), jnp.float32)
    mass_flux = noise(arg_keys[1], (3, LEV, NCELL), 1.0, 6.0, ((2, 32),), jnp.float32)
    lsq_coeff = noise(arg_keys[2], (2, 3, NCELL), 0.5, 3.0, ((2, 32),), jnp.float32)
    own_offset = noise(arg_keys[3], (2, 3, LEV, NCELL), 0.3, 1.5, ((3, 32),), jnp.float32)
    far_offset = noise(arg_keys[4], (2, 3, LEV, NCELL), 0.3, 1.5, ((3, 32),), jnp.float32)
    inv_mass = jnp.clip(jnp.exp(math.log(1.0) - 1.3862944 * jax.random.uniform(arg_keys[5], (LEV, NCELL), jnp.float32) ** steps_of(arg_keys[5], (LEV, NCELL), ((1, 32),), -0.2, 0.2)), 0.25, 1.0)
    neighbour = draw_neighbour(jax.random.fold_in(arg_keys[8], 71), 0)
    send_cells = draw_send_cells(jax.random.fold_in(arg_keys[8], 71), 0)
    return {"tracers": tracers, "mass_flux": mass_flux, "lsq_coeff": lsq_coeff, "own_offset": own_offset, "far_offset": far_offset, "inv_mass": inv_mass, "neighbour": neighbour, "send_cells": send_cells}


def peer_shift(peer_slot):
    return (peer_slot // 2 + 1) * (1 - 2 * (peer_slot % 2))


def reference(tracers, mass_flux, lsq_coeff, own_offset, far_offset, inv_mass, neighbour, send_cells):
    devices = NCELL // CEL_DEV
    offsets = jnp.array([peer_shift(peer_slot) for peer_slot in range(PEERS)], jnp.int32)
    owners = jnp.arange(devices, dtype=jnp.int32)
    sender = ((owners[:, None] - offsets[None, :]) % devices).astype(jnp.int32)
    blocks = send_cells.reshape(PEERS, devices, HALO).astype(jnp.int32)
    remote = blocks[jnp.arange(PEERS, dtype=jnp.int32)[None, :], sender, :]
    remote = (remote + sender[:, :, None] * CEL_DEV).astype(jnp.int32)
    own_ids = (owners[:, None] * CEL_DEV + jnp.arange(CEL_DEV, dtype=jnp.int32)[None, :]).astype(jnp.int32)
    lookup = jnp.concatenate([own_ids, remote.reshape(devices, PEERS * HALO)], axis=1).astype(jnp.int32)
    local_ids = neighbour.reshape(3, devices, CEL_DEV).astype(jnp.int32)
    wide_lookup = jnp.broadcast_to(lookup[None], (3, devices, lookup.shape[1]))
    global_ids = jnp.take_along_axis(wide_lookup, local_ids, axis=2).reshape(3, NCELL).astype(jnp.int32)
    beside = [jnp.take(tracers, global_ids[edge_slot], axis=2) for edge_slot in range(3)]
    gradient = None
    for edge_slot in range(3):
        summand = lsq_coeff[:, edge_slot][:, None, None, :] * (beside[edge_slot] - tracers)[None]
        gradient = summand if gradient is None else gradient + summand
    outflow = jnp.zeros_like(tracers)
    for edge_slot in range(3):
        far_value = beside[edge_slot]
        far_grad = jnp.take(gradient, global_ids[edge_slot], axis=3)
        own_face = tracers + gradient[0] * own_offset[0, edge_slot] + gradient[1] * own_offset[1, edge_slot]
        far_face = far_value + far_grad[0] * far_offset[0, edge_slot] + far_grad[1] * far_offset[1, edge_slot]
        side_flux = mass_flux[edge_slot]
        face_value = jnp.where(side_flux > 0, own_face, far_face)
        face_value = jnp.clip(face_value, jnp.minimum(tracers, far_value), jnp.maximum(tracers, far_value))
        outflow = outflow + side_flux * face_value
    return tracers - inv_mass * outflow
```

```python
import functools

import jax
import jax.numpy as jnp
from jax import lax
from jax.experimental import pallas as pl
from jax.experimental.pallas import tpu as pltpu
from jax.sharding import PartitionSpec as P

MESH = pl.DeviceIdType.MESH
PARTS = (2, 3, 3, 2)
WIDTH = 1536


def peer_shift(peer_slot):
    return (peer_slot // 2 + 1) * (1 - 2 * (peer_slot % 2))


def wrap(position, devices):
    return lax.rem(position + devices, devices)


def leading(me):
    return 0


def lanes(block, width):
    return pl.ds(pl.multiple_of(block * width, width), width)


def split(value):
    high = value.astype(jnp.bfloat16)
    return high, (value - high.astype(jnp.float32)).astype(jnp.bfloat16)


def kernel(
    parts,
    tracers_hbm,
    flux_hbm,
    lsq_hbm,
    own_hbm,
    far_hbm,
    inv_hbm,
    near_hbm,
    send_hbm,
    out,
    tracers,
    flux,
    lsq,
    own_off,
    far_off,
    inv_mass,
    near,
    send_cells,
    load_sem,
    hot,
    send_hot,
    low_x,
    low_g,
    grads,
    beside,
    far,
    value_out,
    value_in,
    grad_out,
    grad_in,
    halo_x,
    halo_g,
    send_sem,
    recv_sem,
    top_sem,
):
    tracer_count, level_count, cells = tracers.shape
    rows = tracer_count * level_count
    peers, halo = send_cells.shape
    ext = cells + peers * halo
    me = lax.axis_index("dom")
    devices = lax.axis_size("dom")
    lead = leading(me)
    f32, bf16 = jnp.float32, jnp.bfloat16
    reach = peers // 2
    order = [q for q in (1, 2, 0) if q < reach] + list(range(3, reach))

    barrier = pltpu.get_barrier_semaphore()
    for p in range(peers):
        to = me + peer_shift(p)

        @pl.when(to < devices)
        def _():
            pl.semaphore_signal(
                barrier, inc=1, device_id=(wrap(to, devices),), device_id_type=MESH
            )

    below = sum([jnp.where(me + peer_shift(p) < 0, 1, 0) for p in range(peers)])

    pairs = (
        (send_hbm, send_cells),
        (tracers_hbm, tracers),
        (near_hbm, near),
        (lsq_hbm, lsq),
        (flux_hbm, flux),
        (own_hbm, own_off),
        (far_hbm, far_off),
        (inv_hbm, inv_mass),
    )
    early = sum(parts[0]) // level_count
    soon, rest = pl.ds(0, early), pl.ds(early, tracer_count - early)
    late = pltpu.make_async_copy(
        tracers_hbm.at[rest], tracers.at[rest], load_sem.at[len(pairs)]
    )
    pairs = pairs[:1] + ((tracers_hbm.at[soon], tracers.at[soon]),) + pairs[2:]
    loads = [pltpu.make_async_copy(a, b, load_sem.at[i]) for i, (a, b) in enumerate(pairs)]
    for load in loads[:2] + [late] + loads[2:]:
        load.start()
    loads[0].wait()

    row = lax.broadcasted_iota(jnp.int32, (16, 128), 0).astype(jnp.int16)
    one, zero = jnp.ones((16, 128), bf16), jnp.zeros((16, 128), bf16)

    def match(table, count, width, dest, height):
        for j in range(count):

            def build(b, carry):
                index = jnp.broadcast_to(table[j : j + 1, lanes(b, 128)], (16, 128))
                index = index.astype(jnp.int16) - row
                cols = pl.ds(pl.multiple_of(j * width + b * 128, 128), 128)
                for r in range(0, height, 16):
                    dest[r : r + 16, cols] = jnp.where(index == jnp.int16(r), one, zero)
                return carry

            lax.fori_loop(0, width // 128, build, 0)

    match(send_cells, peers, halo, send_hot, cells)

    loads[1].wait()

    def split_x(start, count):
        def step(i, carry):
            t = start // level_count + 2 * i
            high, low = split(jnp.concatenate([tracers[t], tracers[t + 1]], axis=0))
            base = 2 * start + 16 * i
            low_x[pl.ds(pl.multiple_of(base, 16), 16), :] = high
            low_x[pl.ds(pl.multiple_of(base + count, 16), 16), :] = low
            return carry

        lax.fori_loop(0, count // 16, step, 0)

    def copy_of(kind, c, p, to):
        src, dst = (value_out, value_in) if kind == 0 else (grad_out, grad_in)
        start, count = [(1 + kind) * v for v in parts[c]]
        return pltpu.make_async_remote_copy(
            src_ref=src.at[p, pl.ds(start, count)],
            dst_ref=dst.at[p, pl.ds(start, count)],
            send_sem=send_sem.at[kind],
            recv_sem=recv_sem.at[kind, c],
            device_id=(wrap(to, devices),),
            device_id_type=MESH,
        )

    def all_of(kind, start, count, c):
        src, dst = (value_out, value_in) if kind == 0 else (grad_out, grad_in)
        return pltpu.make_async_remote_copy(
            src_ref=src.at[:, pl.ds((1 + kind) * start, (1 + kind) * count)],
            dst_ref=dst.at[:, pl.ds((1 + kind) * start, (1 + kind) * count)],
            send_sem=send_sem.at[kind],
            recv_sem=recv_sem.at[kind, c],
            device_id=(wrap(me + 1, devices),),
            device_id_type=MESH,
        )

    def send(kind, c, wanted):
        for side in range(2):
            bit = lead if side == 0 else 1 - lead
            for q in order:
                to = me + (q + 1) * (1 - 2 * bit)
                pl.when(wanted(to))(copy_of(kind, c, 2 * q + bit, to).start)

    def above_ground(to):
        return to >= 0

    def under_ground(to):
        return to < 0

    def late_gradient(to):
        return jnp.logical_or(to < 0, jnp.logical_and(top, to < devices))

    def soon_gradient(to):
        return jnp.logical_not(late_gradient(to))

    def pack(terms, dest, start, count):
        for p in range(0, peers, 2):
            part = jnp.dot(
                terms[pl.ds(2 * start, 2 * count), :],
                send_hot[:, p * halo : (p + 2) * halo],
                preferred_element_type=f32,
            )
            part = part[:count] + part[count:]
            for q in range(2):
                dest[p + q, pl.ds(start, count), :] = part[:, q * halo : (q + 1) * halo]

    def local(terms, dest, scale, first, last):
        def step(b, carry):
            cols = lanes(b, WIDTH)
            part = jnp.dot(terms[...], hot[:cells, cols], preferred_element_type=f32)
            for start, count in parts:
                start, count = scale * start, scale * count
                s = 2 * start
                dest[start : start + count, cols] = (
                    part[s : s + count] + part[s + count : s + 2 * count]
                )
            return carry

        lax.fori_loop(first, last, step, 0)

    def remote(arrived, terms, dest, start, count):
        for p in range(peers):
            high, low = split(arrived[p, pl.ds(start, count), :])
            terms[:count, p * halo : (p + 1) * halo] = high
            terms[count : 2 * count, p * halo : (p + 1) * halo] = low

        def step(b, carry):
            cols = lanes(b, 2 * WIDTH)
            part = jnp.dot(
                terms[: 2 * count, :], hot[cells:ext, cols], preferred_element_type=f32
            )
            dest[start : start + count, cols] += part[:count] + part[count:]
            return carry

        lax.fori_loop(0, 3 * cells // (2 * WIDTH), step, 0)

    def gradient(start, per):
        def step(i, carry):
            t = start // level_count + 2 * i
            r = start + 16 * i
            here = jnp.concatenate([tracers[t], tracers[t + 1]], axis=0)
            at = pl.ds(pl.multiple_of(r, 16), 16)
            delta = [beside[at, j * cells : (j + 1) * cells] - here for j in range(3)]
            for k in range(2):
                total = lsq[0, k : k + 1, :] * delta[0]
                total = total + lsq[1, k : k + 1, :] * delta[1]
                total = total + lsq[2, k : k + 1, :] * delta[2]
                grads[k, at, :] = total
                high, low = split(total)
                base = 4 * start + k * per + 16 * i
                low_g[pl.ds(pl.multiple_of(base, 16), 16), :] = high
                low_g[pl.ds(pl.multiple_of(base + 2 * per, 16), 16), :] = low
            return carry

        lax.fori_loop(0, per // 16, step, 0)

    def finish(start, per):
        def step(i, carry):
            t = start // level_count + i
            at = pl.ds(pl.multiple_of(t * level_count, 8), level_count)
            f0 = pl.ds(pl.multiple_of(2 * start + i * level_count, 8), level_count)
            f1 = pl.ds(pl.multiple_of(2 * start + per + i * level_count, 8), level_count)
            for b in range(cells // 256):
                own = slice(b * 256, (b + 1) * 256)
                here = tracers[t, :, own]
                g0, g1 = grads[0, at, own], grads[1, at, own]
                outflow = None
                for j in range(3):
                    cols = slice(j * cells + b * 256, j * cells + (b + 1) * 256)
                    there = beside[at, cols]
                    own_face = here + g0 * own_off[0, j, :, own] + g1 * own_off[1, j, :, own]
                    far_face = (
                        there
                        + far[f0, cols] * far_off[0, j, :, own]
                        + far[f1, cols] * far_off[1, j, :, own]
                    )
                    side = flux[j, :, own]
                    face = jnp.where(side > 0, own_face, far_face)
                    face = jnp.maximum(face, jnp.minimum(here, there))
                    face = jnp.minimum(face, jnp.maximum(here, there))
                    term = side * face
                    outflow = term if outflow is None else outflow + term
                out[t, :, own] = here - inv_mass[:, own] * outflow
            return carry

        lax.fori_loop(0, per // level_count, step, 0)

    count_parts = len(parts)
    def pack_x(first, last):
        start, stop = parts[first][0], sum(parts[last])
        for part in parts[first : last + 1]:
            split_x(*part)
        whole = jnp.dot(
            low_x[2 * start : 2 * stop, :],
            send_hot[:, : peers * halo],
            preferred_element_type=f32,
        )
        for begin, count in parts[first : last + 1]:
            at = 2 * (begin - start)
            part = whole[at : at + count] + whole[at + count : at + 2 * count]
            for p in range(peers):
                value_out[p, begin : begin + count, :] = part[:, p * halo : (p + 1) * halo]

    top = me + reach >= devices

    def enter():
        pl.semaphore_wait(barrier, peers - below)

    @pl.when(top)
    def _():
        enter()
        for q in range(reach):
            to = me + q + 1

            @pl.when(to >= devices)
            def _():
                pl.semaphore_signal(
                    top_sem, inc=1, device_id=(wrap(to, devices),), device_id_type=MESH
                )

    pack_x(0, 0)
    interior = jnp.logical_not(jnp.logical_or(top, below > 0))
    pl.when(interior)(enter)

    @pl.when(below == 0)
    def _():
        send(0, 0, above_ground)

    late.wait()
    pack_x(1, count_parts - 1)

    @pl.when(below > 0)
    def _():
        enter()
        send(0, 0, above_ground)

    for c in range(1, count_parts):
        send(0, c, above_ground)
    loads[2].wait()
    match(near, 3, cells, hot, ext)
    loads[3].wait()
    local(low_x, beside, 1, 0, 1)

    @pl.when(below > 0)
    def _():
        pl.semaphore_wait(top_sem, below)
        for c in range(count_parts):
            send(0, c, under_ground)

    local(low_x, beside, 1, 1, 3 * cells // WIDTH)
    for c in range(count_parts):
        start, count = parts[c]
        all_of(0, start, count, c).wait_recv()
        remote(value_in, halo_x, beside, start, count)
        gradient(start, count)
        pack(low_g, grad_out, 2 * start, 2 * count)
        send(1, c, soon_gradient)
    for c in range(count_parts):
        send(1, c, late_gradient)
    local(low_g, far, 2, 0, 3 * cells // WIDTH)
    for load in loads[4:]:
        load.wait()
    for c in range(count_parts):
        start, count = parts[c]
        all_of(1, start, count, c).wait_recv()
        remote(grad_in, halo_g, far, 2 * start, 2 * count)
        finish(start, count)
    for kind in range(2):
        all_of(kind, 0, rows, 0).wait_send()


def on_device(tracers, flux, lsq, own_off, far_off, inv_mass, near, send_cells):
    tracer_count, level_count, cells = tracers.shape
    rows = tracer_count * level_count
    peers, halo = send_cells.shape
    sizes = PARTS if 16 * sum(PARTS) == rows else (rows // 16,)
    parts, start = [], 0
    for size in sizes:
        parts.append((start, 16 * size))
        start += 16 * size
    per = 16 * max(sizes)
    lsq = lsq.transpose(1, 0, 2)
    operands = (tracers, flux, lsq, own_off, far_off, inv_mass, near, send_cells)
    ext = cells + peers * halo
    f32, bf16 = jnp.float32, jnp.bfloat16
    return pl.pallas_call(
        functools.partial(kernel, parts),
        out_shape=jax.ShapeDtypeStruct(tracers.shape, f32),
        in_specs=[pl.BlockSpec(memory_space=pltpu.HBM)] * 8,
        out_specs=pl.BlockSpec(memory_space=pltpu.VMEM),
        scratch_shapes=[pltpu.VMEM(a.shape, a.dtype) for a in operands]
        + [
            pltpu.SemaphoreType.DMA((9,)),
            pltpu.VMEM((ext, 3 * cells + 128), bf16),
            pltpu.VMEM((cells, peers * halo + 128), bf16),
            pltpu.VMEM((2 * rows, cells), bf16),
            pltpu.VMEM((4 * rows, cells), bf16),
            pltpu.VMEM((2, rows, cells), f32),
            pltpu.VMEM((rows, 3 * cells), f32),
            pltpu.VMEM((2 * rows, 3 * cells), f32),
            pltpu.VMEM((peers, rows, halo), f32),
            pltpu.VMEM((peers, rows, halo), f32),
            pltpu.VMEM((peers, 2 * rows, halo), f32),
            pltpu.VMEM((peers, 2 * rows, halo), f32),
            pltpu.VMEM((2 * per, peers * halo), bf16),
            pltpu.VMEM((4 * per, peers * halo), bf16),
            pltpu.SemaphoreType.DMA((2,)),
            pltpu.SemaphoreType.DMA((2, len(parts))),
            pltpu.SemaphoreType.REGULAR,
        ],
        compiler_params=pltpu.CompilerParams(
            collective_id=0, has_side_effects=True, vmem_limit_bytes=40 * 1024 * 1024
        ),
        name="step",
    )(*[pltpu.with_memory_space_constraint(a, pltpu.HBM) for a in operands])


def solution(mesh):
    placed = (
        P(None, None, "dom"),
        P(None, None, "dom"),
        P(None, None, "dom"),
        P(None, None, None, "dom"),
        P(None, None, None, "dom"),
        P(None, "dom"),
        P(None, "dom"),
        P(None, "dom"),
    )
    return jax.shard_map(
        on_device, mesh=mesh, in_specs=placed, out_specs=P(None, None, "dom"), check_vma=False
    )
```

```python
import functools

import jax
import jax.numpy as jnp
from jax import lax
from jax.experimental import pallas as pl
from jax.experimental.pallas import tpu as pltpu
from jax.sharding import PartitionSpec as P

MESH = pl.DeviceIdType.MESH
PARTS = (2, 2, 3, 2, 1)
WIDTH = 1536
ONE_HOT = jnp.float8_e4m3fn


def peer_shift(peer_slot):
    return (peer_slot // 2 + 1) * (1 - 2 * (peer_slot % 2))


def wrap(position, devices):
    return lax.rem(position + devices, devices)


def leading(me):
    return 0


def lanes(block, width):
    return pl.ds(pl.multiple_of(block * width, width), width)


def pick(terms, one_hot):
    return lax.dot_general(
        terms, one_hot, (((1,), (0,)), ((), ())), preferred_element_type=jnp.float32
    )


def split(value):
    high = value.astype(jnp.bfloat16)
    return high, (value - high.astype(jnp.float32)).astype(jnp.bfloat16)


def kernel(
    parts,
    tracers_hbm,
    flux_hbm,
    lsq_hbm,
    own_hbm,
    far_hbm,
    inv_hbm,
    near_hbm,
    send_hbm,
    out,
    tracers,
    flux,
    lsq,
    own_off,
    far_off,
    inv_mass,
    near,
    send_cells,
    load_sem,
    hot,
    send_hot,
    low_x,
    low_g,
    grads,
    beside,
    far,
    value_out,
    value_in,
    grad_out,
    grad_in,
    halo_x,
    halo_g,
    send_sem,
    recv_sem,
    top_sem,
):
    tracer_count, level_count, cells = tracers.shape
    rows = tracer_count * level_count
    peers, halo = send_cells.shape
    ext = cells + peers * halo
    me = lax.axis_index("dom")
    devices = lax.axis_size("dom")
    lead = leading(me)
    f32, bf16 = jnp.float32, jnp.bfloat16
    reach = peers // 2
    order = [q for q in (1, 2, 0) if q < reach] + list(range(3, reach))

    barrier = pltpu.get_barrier_semaphore()
    for p in range(peers):
        to = me + peer_shift(p)

        @pl.when(to < devices)
        def _():
            pl.semaphore_signal(
                barrier, inc=1, device_id=(wrap(to, devices),), device_id_type=MESH
            )

    below = sum([jnp.where(me + peer_shift(p) < 0, 1, 0) for p in range(peers)])

    pairs = (
        (send_hbm, send_cells),
        (tracers_hbm, tracers),
        (near_hbm, near),
        (lsq_hbm, lsq),
        (flux_hbm, flux),
        (own_hbm, own_off),
        (far_hbm, far_off),
        (inv_hbm, inv_mass),
    )
    early = sum(parts[0]) // level_count
    soon, rest = pl.ds(0, early), pl.ds(early, tracer_count - early)
    late = pltpu.make_async_copy(
        tracers_hbm.at[rest], tracers.at[rest], load_sem.at[len(pairs)]
    )
    pairs = pairs[:1] + ((tracers_hbm.at[soon], tracers.at[soon]),) + pairs[2:]
    loads = [pltpu.make_async_copy(a, b, load_sem.at[i]) for i, (a, b) in enumerate(pairs)]
    for load in loads[:2] + [late] + loads[2:]:
        load.start()
    top = me + reach >= devices

    def enter():
        pl.semaphore_wait(barrier, peers - below)

    @pl.when(top)
    def _():
        enter()
        for q in range(reach):
            to = me + q + 1

            @pl.when(to >= devices)
            def _():
                pl.semaphore_signal(
                    top_sem.at[q], inc=1, device_id=(wrap(to, devices),), device_id_type=MESH
                )

    loads[0].wait()

    row = lax.broadcasted_iota(jnp.int32, (32, 128), 0).astype(jnp.int16)
    one, zero = jnp.ones((32, 128), bf16), jnp.zeros((32, 128), bf16)

    def match(table, count, width, dest, height):
        for j in range(count):

            def build(b, carry):
                index = jnp.broadcast_to(table[j : j + 1, lanes(b, 128)], (32, 128))
                index = index.astype(jnp.int16) - row
                cols = pl.ds(pl.multiple_of(j * width + b * 128, 128), 128)
                for r in range(0, height, 32):
                    hit = jnp.where(index == jnp.int16(r), one, zero)
                    dest[r : r + 32, cols] = hit.astype(dest.dtype)
                return carry

            lax.fori_loop(0, width // 128, build, 0)

    match(send_cells, peers, halo, send_hot, cells)

    loads[1].wait()

    def split_x(start, count):
        def step(i, carry):
            t = start // level_count + 2 * i
            high, low = split(jnp.concatenate([tracers[t], tracers[t + 1]], axis=0))
            base = 2 * start + 16 * i
            low_x[pl.ds(pl.multiple_of(base, 16), 16), :] = high
            low_x[pl.ds(pl.multiple_of(base + count, 16), 16), :] = low
            return carry

        lax.fori_loop(0, count // 16, step, 0)

    def copy_of(kind, c, p, to):
        src, dst = (value_out, value_in) if kind == 0 else (grad_out, grad_in)
        start, count = [(1 + kind) * v for v in parts[c]]
        return pltpu.make_async_remote_copy(
            src_ref=src.at[p, pl.ds(start, count)],
            dst_ref=dst.at[p, pl.ds(start, count)],
            send_sem=send_sem.at[kind],
            recv_sem=recv_sem.at[kind, c],
            device_id=(wrap(to, devices),),
            device_id_type=MESH,
        )

    def all_of(kind, start, count, c):
        src, dst = (value_out, value_in) if kind == 0 else (grad_out, grad_in)
        return pltpu.make_async_remote_copy(
            src_ref=src.at[:, pl.ds((1 + kind) * start, (1 + kind) * count)],
            dst_ref=dst.at[:, pl.ds((1 + kind) * start, (1 + kind) * count)],
            send_sem=send_sem.at[kind],
            recv_sem=recv_sem.at[kind, c],
            device_id=(wrap(me + 1, devices),),
            device_id_type=MESH,
        )

    def send(kind, c, wanted):
        for side in range(2):
            bit = lead if side == 0 else 1 - lead
            for q in order:
                to = me + (q + 1) * (1 - 2 * bit)
                pl.when(wanted(to))(copy_of(kind, c, 2 * q + bit, to).start)

    def above_ground(to):
        return to >= 0

    def under_ground(to):
        return to < 0

    def late_gradient(to):
        last = me + reach + 1 >= devices
        return (to < 0) | (top & (to < devices)) | (last & (to == me - reach))

    def soon_gradient(to):
        return jnp.logical_not(late_gradient(to))

    def pack(terms, dest, start, count):
        for p in range(0, peers, 2):
            part = pick(
                terms[pl.ds(2 * start, 2 * count), :], send_hot[:, p * halo : (p + 2) * halo]
            )
            part = part[:count] + part[count:]
            for q in range(2):
                dest[p + q, pl.ds(start, count), :] = part[:, q * halo : (q + 1) * halo]

    def local(terms, dest, scale, first, last):
        def step(b, carry):
            cols = lanes(b, WIDTH)
            part = pick(terms[...], hot[:cells, cols])
            for start, count in parts:
                start, count = scale * start, scale * count
                s = 2 * start
                dest[start : start + count, cols] = (
                    part[s : s + count] + part[s + count : s + 2 * count]
                )
            return carry

        lax.fori_loop(first, last, step, 0)

    def remote(arrived, terms, dest, start, count):
        for p in range(peers):
            high, low = split(arrived[p, pl.ds(start, count), :])
            terms[:count, p * halo : (p + 1) * halo] = high
            terms[count : 2 * count, p * halo : (p + 1) * halo] = low

        def step(b, carry):
            cols = lanes(b, 2 * WIDTH)
            part = pick(terms[: 2 * count, :], hot[cells:ext, cols])
            dest[start : start + count, cols] += part[:count] + part[count:]
            return carry

        lax.fori_loop(0, 3 * cells // (2 * WIDTH), step, 0)

    def gradient(start, per):
        def step(i, carry):
            t = start // level_count + 2 * i
            r = start + 16 * i
            here = jnp.concatenate([tracers[t], tracers[t + 1]], axis=0)
            at = pl.ds(pl.multiple_of(r, 16), 16)
            delta = [beside[at, j * cells : (j + 1) * cells] - here for j in range(3)]
            for k in range(2):
                total = lsq[0, k : k + 1, :] * delta[0]
                total = total + lsq[1, k : k + 1, :] * delta[1]
                total = total + lsq[2, k : k + 1, :] * delta[2]
                grads[k, at, :] = total
                high, low = split(total)
                base = 4 * start + k * per + 16 * i
                low_g[pl.ds(pl.multiple_of(base, 16), 16), :] = high
                low_g[pl.ds(pl.multiple_of(base + 2 * per, 16), 16), :] = low
            return carry

        lax.fori_loop(0, per // 16, step, 0)

    def finish(start, per):
        def step(i, carry):
            t = start // level_count + i
            at = pl.ds(pl.multiple_of(t * level_count, 8), level_count)
            f0 = pl.ds(pl.multiple_of(2 * start + i * level_count, 8), level_count)
            f1 = pl.ds(pl.multiple_of(2 * start + per + i * level_count, 8), level_count)
            for b in range(cells // 256):
                own = slice(b * 256, (b + 1) * 256)
                here = tracers[t, :, own]
                g0, g1 = grads[0, at, own], grads[1, at, own]
                outflow = None
                for j in range(3):
                    cols = slice(j * cells + b * 256, j * cells + (b + 1) * 256)
                    there = beside[at, cols]
                    own_face = here + g0 * own_off[0, j, :, own] + g1 * own_off[1, j, :, own]
                    far_face = (
                        there
                        + far[f0, cols] * far_off[0, j, :, own]
                        + far[f1, cols] * far_off[1, j, :, own]
                    )
                    side = flux[j, :, own]
                    face = jnp.where(side > 0, own_face, far_face)
                    face = jnp.maximum(face, jnp.minimum(here, there))
                    face = jnp.minimum(face, jnp.maximum(here, there))
                    term = side * face
                    outflow = term if outflow is None else outflow + term
                out[t, :, own] = here - inv_mass[:, own] * outflow
            return carry

        lax.fori_loop(0, per // level_count, step, 0)

    count_parts = len(parts)
    def pack_x(first, last):
        start, stop = parts[first][0], sum(parts[last])
        for part in parts[first : last + 1]:
            split_x(*part)
        whole = pick(low_x[2 * start : 2 * stop, :], send_hot[:, : peers * halo])
        for begin, count in parts[first : last + 1]:
            at = 2 * (begin - start)
            part = whole[at : at + count] + whole[at + count : at + 2 * count]
            for p in range(peers):
                value_out[p, begin : begin + count, :] = part[:, p * halo : (p + 1) * halo]

    pack_x(0, 0)
    interior = jnp.logical_not(jnp.logical_or(top, below > 0))
    pl.when(interior)(enter)

    @pl.when(below == 0)
    def _():
        send(0, 0, above_ground)

    late.wait()
    pack_x(1, count_parts - 1)

    @pl.when(below > 0)
    def _():
        enter()
        send(0, 0, above_ground)

    for c in range(1, count_parts):
        send(0, c, above_ground)
    loads[2].wait()
    match(near, 3, cells, hot, ext)
    loads[3].wait()
    local(low_x, beside, 1, 0, 1)

    @pl.when(below > 0)
    def _():
        for q in order[::-1]:
            to = me - q - 1

            @pl.when(to < 0)
            def _():
                pl.semaphore_wait(top_sem.at[q], 1)
                copy_of(0, 0, 2 * q + 1, to).start()

        for c in range(1, count_parts):
            send(0, c, under_ground)

    local(low_x, beside, 1, 1, 3 * cells // WIDTH)
    for c in range(count_parts):
        start, count = parts[c]
        all_of(0, start, count, c).wait_recv()
        remote(value_in, halo_x, beside, start, count)
        gradient(start, count)
        pack(low_g, grad_out, 2 * start, 2 * count)
        send(1, c, soon_gradient)
    for c in range(count_parts):
        send(1, c, late_gradient)
    local(low_g, far, 2, 0, 3 * cells // WIDTH)
    for load in loads[4:]:
        load.wait()
    for c in range(count_parts):
        start, count = parts[c]
        all_of(1, start, count, c).wait_recv()
        remote(grad_in, halo_g, far, 2 * start, 2 * count)
        finish(start, count)
    for kind in range(2):
        all_of(kind, 0, rows, 0).wait_send()


def on_device(tracers, flux, lsq, own_off, far_off, inv_mass, near, send_cells):
    tracer_count, level_count, cells = tracers.shape
    rows = tracer_count * level_count
    peers, halo = send_cells.shape
    sizes = PARTS if 16 * sum(PARTS) == rows else (rows // 16,)
    parts, start = [], 0
    for size in sizes:
        parts.append((start, 16 * size))
        start += 16 * size
    per = 16 * max(sizes)
    lsq = lsq.transpose(1, 0, 2)
    operands = (tracers, flux, lsq, own_off, far_off, inv_mass, near, send_cells)
    ext = cells + peers * halo
    f32, bf16 = jnp.float32, jnp.bfloat16
    return pl.pallas_call(
        functools.partial(kernel, parts),
        out_shape=jax.ShapeDtypeStruct(tracers.shape, f32),
        in_specs=[pl.BlockSpec(memory_space=pltpu.HBM)] * 8,
        out_specs=pl.BlockSpec(memory_space=pltpu.VMEM),
        scratch_shapes=[pltpu.VMEM(a.shape, a.dtype) for a in operands]
        + [
            pltpu.SemaphoreType.DMA((9,)),
            pltpu.VMEM((ext, 3 * cells + 128), ONE_HOT),
            pltpu.VMEM((cells, peers * halo + 128), ONE_HOT),
            pltpu.VMEM((2 * rows, cells), bf16),
            pltpu.VMEM((4 * rows, cells), bf16),
            pltpu.VMEM((2, rows, cells), f32),
            pltpu.VMEM((rows, 3 * cells), f32),
            pltpu.VMEM((2 * rows, 3 * cells), f32),
            pltpu.VMEM((peers, rows, halo), f32),
            pltpu.VMEM((peers, rows, halo), f32),
            pltpu.VMEM((peers, 2 * rows, halo), f32),
            pltpu.VMEM((peers, 2 * rows, halo), f32),
            pltpu.VMEM((2 * per, peers * halo), bf16),
            pltpu.VMEM((4 * per, peers * halo), bf16),
            pltpu.SemaphoreType.DMA((2,)),
            pltpu.SemaphoreType.DMA((2, len(parts))),
            pltpu.SemaphoreType.REGULAR((peers // 2,)),
        ],
        compiler_params=pltpu.CompilerParams(
            collective_id=0, has_side_effects=True, vmem_limit_bytes=40 * 1024 * 1024
        ),
        name="step",
    )(*[pltpu.with_memory_space_constraint(a, pltpu.HBM) for a in operands])


def solution(mesh):
    placed = (
        P(None, None, "dom"),
        P(None, None, "dom"),
        P(None, None, "dom"),
        P(None, None, None, "dom"),
        P(None, None, None, "dom"),
        P(None, "dom"),
        P(None, "dom"),
        P(None, "dom"),
    )
    return jax.shard_map(
        on_device, mesh=mesh, in_specs=placed, out_specs=P(None, None, "dom"), check_vma=False
    )
```

```python
import functools

import jax
import jax.numpy as jnp
from jax import lax
from jax.experimental import pallas as pl
from jax.experimental.pallas import tpu as pltpu
from jax.sharding import PartitionSpec as P

MESH = pl.DeviceIdType.MESH
PARTS = (2, 2, 2, 2, 1, 1)
WIDTH = 1536
ONE_HOT = jnp.float8_e4m3fn


def peer_shift(peer_slot):
    return (peer_slot // 2 + 1) * (1 - 2 * (peer_slot % 2))


def wrap(position, devices):
    return lax.rem(position + devices, devices)


def lanes(block, width):
    return pl.ds(pl.multiple_of(block * width, width), width)


def pick(terms, one_hot):
    return lax.dot_general(
        terms, one_hot, (((1,), (0,)), ((), ())), preferred_element_type=jnp.float32
    )


def split(value):
    high = value.astype(jnp.bfloat16)
    return high, (value - high.astype(jnp.float32)).astype(jnp.bfloat16)


def kernel(
    parts,
    tracers_hbm,
    flux_hbm,
    lsq_hbm,
    own_hbm,
    far_hbm,
    inv_hbm,
    near_hbm,
    send_hbm,
    out,
    tracers,
    flux,
    lsq,
    own_off,
    far_off,
    inv_mass,
    near,
    send_cells,
    load_sem,
    hot,
    send_hot,
    low_x,
    low_g,
    grads,
    beside,
    far,
    value_out,
    value_in,
    grad_out,
    grad_in,
    halo_x,
    halo_g,
    send_sem,
    recv_sem,
    top_sem,
):
    tracer_count, level_count, cells = tracers.shape
    rows = tracer_count * level_count
    peers, halo = send_cells.shape
    ext = cells + peers * halo
    me = lax.axis_index("dom")
    devices = lax.axis_size("dom")
    f32, bf16 = jnp.float32, jnp.bfloat16
    reach = peers // 2
    order = [q for q in (1, 2, 0) if q < reach] + list(range(3, reach))

    barrier = pltpu.get_barrier_semaphore()
    for p in range(peers):
        to = me + peer_shift(p)

        @pl.when(to < devices)
        def _():
            pl.semaphore_signal(
                barrier, inc=1, device_id=(wrap(to, devices),), device_id_type=MESH
            )

    below = sum([jnp.where(me + peer_shift(p) < 0, 1, 0) for p in range(peers)])

    pairs = (
        (send_hbm, send_cells),
        (tracers_hbm, tracers),
        (near_hbm, near),
        (lsq_hbm, lsq),
        (flux_hbm, flux),
        (own_hbm, own_off),
        (far_hbm, far_off),
        (inv_hbm, inv_mass),
    )
    early = sum(parts[0]) // level_count
    soon, rest = pl.ds(0, early), pl.ds(early, tracer_count - early)
    late = pltpu.make_async_copy(
        tracers_hbm.at[rest], tracers.at[rest], load_sem.at[len(pairs)]
    )
    pairs = pairs[:1] + ((tracers_hbm.at[soon], tracers.at[soon]),) + pairs[2:]
    loads = [pltpu.make_async_copy(a, b, load_sem.at[i]) for i, (a, b) in enumerate(pairs)]
    for load in loads[:2] + [late] + loads[2:]:
        load.start()
    top = me + reach >= devices

    def enter():
        pl.semaphore_wait(barrier, peers - below)

    @pl.when(top)
    def _():
        enter()
        for q in range(reach):
            to = me + q + 1

            @pl.when(to >= devices)
            def _():
                pl.semaphore_signal(
                    top_sem.at[q], inc=1, device_id=(wrap(to, devices),), device_id_type=MESH
                )

    loads[0].wait()

    row = lax.broadcasted_iota(jnp.int32, (32, 128), 0).astype(jnp.int16)
    one, zero = jnp.ones((32, 128), bf16), jnp.zeros((32, 128), bf16)

    def match(table, count, width, dest, height):
        for j in range(count):

            def build(b, carry):
                index = jnp.broadcast_to(table[j : j + 1, lanes(b, 128)], (32, 128))
                index = index.astype(jnp.int16) - row
                cols = pl.ds(pl.multiple_of(j * width + b * 128, 128), 128)
                for r in range(0, height, 32):
                    hit = jnp.where(index == jnp.int16(r), one, zero)
                    dest[r : r + 32, cols] = hit.astype(dest.dtype)
                return carry

            lax.fori_loop(0, width // 128, build, 0)

    match(send_cells, peers, halo, send_hot, cells)

    loads[1].wait()

    def split_x(start, count):
        def step(i, carry):
            t = start // level_count + 2 * i
            high, low = split(jnp.concatenate([tracers[t], tracers[t + 1]], axis=0))
            base = 2 * start + 16 * i
            low_x[pl.ds(pl.multiple_of(base, 16), 16), :] = high
            low_x[pl.ds(pl.multiple_of(base + count, 16), 16), :] = low
            return carry

        lax.fori_loop(0, count // 16, step, 0)

    def copy_of(kind, c, p, to):
        src, dst = (value_out, value_in) if kind == 0 else (grad_out, grad_in)
        start, count = [(1 + kind) * v for v in parts[c]]
        return pltpu.make_async_remote_copy(
            src_ref=src.at[p, pl.ds(start, count)],
            dst_ref=dst.at[p, pl.ds(start, count)],
            send_sem=send_sem.at[kind],
            recv_sem=recv_sem.at[kind, c],
            device_id=(wrap(to, devices),),
            device_id_type=MESH,
        )

    def all_of(kind, start, count, c):
        src, dst = (value_out, value_in) if kind == 0 else (grad_out, grad_in)
        return pltpu.make_async_remote_copy(
            src_ref=src.at[:, pl.ds((1 + kind) * start, (1 + kind) * count)],
            dst_ref=dst.at[:, pl.ds((1 + kind) * start, (1 + kind) * count)],
            send_sem=send_sem.at[kind],
            recv_sem=recv_sem.at[kind, c],
            device_id=(wrap(me + 1, devices),),
            device_id_type=MESH,
        )

    def send(kind, c, wanted):
        for bit in range(2):
            for q in order:
                to = me + (q + 1) * (1 - 2 * bit)
                copy = copy_of(kind, c, 2 * q + bit, to)
                if wanted is None:
                    copy.start()
                else:
                    pl.when(wanted(to))(copy.start)

    def above_ground(to):
        return to >= 0

    def under_ground(to):
        return to < 0

    def pack(terms, dest, start, count):
        for p in range(0, peers, 2):
            part = pick(
                terms[pl.ds(2 * start, 2 * count), :], send_hot[:, p * halo : (p + 2) * halo]
            )
            part = part[:count] + part[count:]
            for q in range(2):
                dest[p + q, pl.ds(start, count), :] = part[:, q * halo : (q + 1) * halo]

    def local(terms, dest, scale, first, last):
        def step(b, carry):
            cols = lanes(b, WIDTH)
            part = pick(terms[...], hot[:cells, cols])
            for start, count in parts:
                start, count = scale * start, scale * count
                s = 2 * start
                dest[start : start + count, cols] = (
                    part[s : s + count] + part[s + count : s + 2 * count]
                )
            return carry

        lax.fori_loop(first, last, step, 0)

    def remote(arrived, terms, dest, start, count):
        for p in range(peers):
            high, low = split(arrived[p, pl.ds(start, count), :])
            terms[:count, p * halo : (p + 1) * halo] = high
            terms[count : 2 * count, p * halo : (p + 1) * halo] = low

        def step(b, carry):
            cols = lanes(b, 2 * WIDTH)
            part = pick(terms[: 2 * count, :], hot[cells:ext, cols])
            dest[start : start + count, cols] += part[:count] + part[count:]
            return carry

        lax.fori_loop(0, 3 * cells // (2 * WIDTH), step, 0)

    def gradient(start, per):
        def step(i, carry):
            t = start // level_count + 2 * i
            r = start + 16 * i
            here = jnp.concatenate([tracers[t], tracers[t + 1]], axis=0)
            at = pl.ds(pl.multiple_of(r, 16), 16)
            delta = [beside[at, j * cells : (j + 1) * cells] - here for j in range(3)]
            for k in range(2):
                total = lsq[0, k : k + 1, :] * delta[0]
                total = total + lsq[1, k : k + 1, :] * delta[1]
                total = total + lsq[2, k : k + 1, :] * delta[2]
                grads[k, at, :] = total
                high, low = split(total)
                base = 4 * start + k * per + 16 * i
                low_g[pl.ds(pl.multiple_of(base, 16), 16), :] = high
                low_g[pl.ds(pl.multiple_of(base + 2 * per, 16), 16), :] = low
            return carry

        lax.fori_loop(0, per // 16, step, 0)

    def finish(start, per):
        def step(i, carry):
            t = start // level_count + i
            at = pl.ds(pl.multiple_of(t * level_count, 8), level_count)
            f0 = pl.ds(pl.multiple_of(2 * start + i * level_count, 8), level_count)
            f1 = pl.ds(pl.multiple_of(2 * start + per + i * level_count, 8), level_count)
            for b in range(cells // 256):
                own = slice(b * 256, (b + 1) * 256)
                here = tracers[t, :, own]
                g0, g1 = grads[0, at, own], grads[1, at, own]
                outflow = None
                for j in range(3):
                    cols = slice(j * cells + b * 256, j * cells + (b + 1) * 256)
                    there = beside[at, cols]
                    own_face = here + g0 * own_off[0, j, :, own] + g1 * own_off[1, j, :, own]
                    far_face = (
                        there
                        + far[f0, cols] * far_off[0, j, :, own]
                        + far[f1, cols] * far_off[1, j, :, own]
                    )
                    side = flux[j, :, own]
                    face = jnp.where(side > 0, own_face, far_face)
                    face = jnp.maximum(face, jnp.minimum(here, there))
                    face = jnp.minimum(face, jnp.maximum(here, there))
                    term = side * face
                    outflow = term if outflow is None else outflow + term
                out[t, :, own] = here - inv_mass[:, own] * outflow
            return carry

        lax.fori_loop(0, per // level_count, step, 0)

    count_parts = len(parts)
    def pack_x(first, last):
        start, stop = parts[first][0], sum(parts[last])
        for part in parts[first : last + 1]:
            split_x(*part)
        whole = pick(low_x[2 * start : 2 * stop, :], send_hot[:, : peers * halo])
        for begin, count in parts[first : last + 1]:
            at = 2 * (begin - start)
            part = whole[at : at + count] + whole[at + count : at + 2 * count]
            for p in range(peers):
                value_out[p, begin : begin + count, :] = part[:, p * halo : (p + 1) * halo]

    pack_x(0, 0)
    interior = jnp.logical_not(jnp.logical_or(top, below > 0))
    pl.when(interior)(enter)

    @pl.when(below == 0)
    def _():
        send(0, 0, above_ground)

    late.wait()
    pack_x(1, count_parts - 1)

    @pl.when(below > 0)
    def _():
        enter()
        send(0, 0, above_ground)

    for c in range(1, count_parts):
        send(0, c, above_ground)
    loads[2].wait()
    match(near, 3, cells, hot, ext)
    loads[3].wait()
    local(low_x, beside, 1, 0, 1)

    @pl.when(below > 0)
    def _():
        for q in order[::-1]:
            to = me - q - 1

            @pl.when(to < 0)
            def _():
                pl.semaphore_wait(top_sem.at[q], 1)
                copy_of(0, 0, 2 * q + 1, to).start()

        for c in range(1, count_parts):
            send(0, c, under_ground)

    local(low_x, beside, 1, 1, 3 * cells // WIDTH)
    for c in range(count_parts):
        start, count = parts[c]
        all_of(0, start, count, c).wait_recv()
        remote(value_in, halo_x, beside, start, count)
        gradient(start, count)
        pack(low_g, grad_out, 2 * start, 2 * count)
        send(1, c, None)
    local(low_g, far, 2, 0, 3 * cells // WIDTH)
    for load in loads[4:]:
        load.wait()
    for c in range(count_parts):
        start, count = parts[c]
        all_of(1, start, count, c).wait_recv()
        remote(grad_in, halo_g, far, 2 * start, 2 * count)
        finish(start, count)
    for kind in range(2):
        all_of(kind, 0, rows, 0).wait_send()


def on_device(tracers, flux, lsq, own_off, far_off, inv_mass, near, send_cells):
    tracer_count, level_count, cells = tracers.shape
    rows = tracer_count * level_count
    peers, halo = send_cells.shape
    sizes = PARTS if 16 * sum(PARTS) == rows else (rows // 16,)
    parts, start = [], 0
    for size in sizes:
        parts.append((start, 16 * size))
        start += 16 * size
    per = 16 * max(sizes)
    lsq = lsq.transpose(1, 0, 2)
    operands = (tracers, flux, lsq, own_off, far_off, inv_mass, near, send_cells)
    ext = cells + peers * halo
    f32, bf16 = jnp.float32, jnp.bfloat16
    return pl.pallas_call(
        functools.partial(kernel, parts),
        out_shape=jax.ShapeDtypeStruct(tracers.shape, f32),
        in_specs=[pl.BlockSpec(memory_space=pltpu.HBM)] * 8,
        out_specs=pl.BlockSpec(memory_space=pltpu.VMEM),
        scratch_shapes=[pltpu.VMEM(a.shape, a.dtype) for a in operands]
        + [
            pltpu.SemaphoreType.DMA((9,)),
            pltpu.VMEM((ext, 3 * cells + 128), ONE_HOT),
            pltpu.VMEM((cells, peers * halo + 128), ONE_HOT),
            pltpu.VMEM((2 * rows, cells), bf16),
            pltpu.VMEM((4 * rows, cells), bf16),
            pltpu.VMEM((2, rows, cells), f32),
            pltpu.VMEM((rows, 3 * cells), f32),
            pltpu.VMEM((2 * rows, 3 * cells), f32),
            pltpu.VMEM((peers, rows, halo), f32),
            pltpu.VMEM((peers, rows, halo), f32),
            pltpu.VMEM((peers, 2 * rows, halo), f32),
            pltpu.VMEM((peers, 2 * rows, halo), f32),
            pltpu.VMEM((2 * per, peers * halo), bf16),
            pltpu.VMEM((4 * per, peers * halo), bf16),
            pltpu.SemaphoreType.DMA((2,)),
            pltpu.SemaphoreType.DMA((2, len(parts))),
            pltpu.SemaphoreType.REGULAR((peers // 2,)),
        ],
        compiler_params=pltpu.CompilerParams(
            collective_id=0, has_side_effects=True, vmem_limit_bytes=40 * 1024 * 1024
        ),
        name="step",
    )(*[pltpu.with_memory_space_constraint(a, pltpu.HBM) for a in operands])


def solution(mesh):
    placed = (
        P(None, None, "dom"),
        P(None, None, "dom"),
        P(None, None, "dom"),
        P(None, None, None, "dom"),
        P(None, None, None, "dom"),
        P(None, "dom"),
        P(None, "dom"),
        P(None, "dom"),
    )
    return jax.shard_map(
        on_device, mesh=mesh, in_specs=placed, out_specs=P(None, None, "dom"), check_vma=False
    )
```

```python
import functools

import jax
import jax.numpy as jnp
from jax import lax
from jax.experimental import pallas as pl
from jax.experimental.pallas import tpu as pltpu
from jax.sharding import PartitionSpec as P

MESH = pl.DeviceIdType.MESH
PARTS = (2, 2, 2, 2, 1, 1)
WIDTH = 1536
ONE_HOT = jnp.float8_e4m3fn


def peer_shift(peer_slot):
    return (peer_slot // 2 + 1) * (1 - 2 * (peer_slot % 2))


def wrap(position, devices):
    return lax.rem(position + devices, devices)


def lanes(block, width):
    return pl.ds(pl.multiple_of(block * width, width), width)


def pick(terms, one_hot):
    return lax.dot_general(
        terms, one_hot, (((1,), (0,)), ((), ())), preferred_element_type=jnp.float32
    )


def split(value):
    high = value.astype(jnp.bfloat16)
    return high, (value - high.astype(jnp.float32)).astype(jnp.bfloat16)


def kernel(
    parts,
    tracers_hbm,
    flux_hbm,
    lsq_hbm,
    own_hbm,
    far_hbm,
    inv_hbm,
    near_hbm,
    send_hbm,
    out,
    tracers,
    flux,
    lsq,
    own_off,
    far_off,
    inv_mass,
    near,
    send_cells,
    load_sem,
    hot,
    send_hot,
    low_x,
    low_g,
    grads,
    beside,
    far,
    value_out,
    value_in,
    grad_out,
    grad_in,
    halo_x,
    halo_g,
    send_sem,
    recv_sem,
    top_sem,
):
    tracer_count, level_count, cells = tracers.shape
    rows = tracer_count * level_count
    peers, halo = send_cells.shape
    ext = cells + peers * halo
    me = lax.axis_index("dom")
    devices = lax.axis_size("dom")
    f32, bf16 = jnp.float32, jnp.bfloat16
    reach = peers // 2
    order = [q for q in (1, 2, 0) if q < reach] + list(range(3, reach))

    barrier = pltpu.get_barrier_semaphore()
    for p in range(peers):
        to = me + peer_shift(p)

        @pl.when(to < devices)
        def _():
            pl.semaphore_signal(
                barrier, inc=1, device_id=(wrap(to, devices),), device_id_type=MESH
            )

    below = sum([jnp.where(me + peer_shift(p) < 0, 1, 0) for p in range(peers)])

    pairs = (
        (send_hbm, send_cells),
        (tracers_hbm, tracers),
        (near_hbm, near),
        (lsq_hbm, lsq),
        (flux_hbm, flux),
        (own_hbm, own_off),
        (far_hbm, far_off),
        (inv_hbm, inv_mass),
    )
    early = sum(parts[0]) // level_count
    soon, rest = pl.ds(0, early), pl.ds(early, tracer_count - early)
    late = pltpu.make_async_copy(
        tracers_hbm.at[rest], tracers.at[rest], load_sem.at[len(pairs)]
    )
    pairs = pairs[:1] + ((tracers_hbm.at[soon], tracers.at[soon]),) + pairs[2:]
    loads = [pltpu.make_async_copy(a, b, load_sem.at[i]) for i, (a, b) in enumerate(pairs)]
    for load in loads[:2] + [late] + loads[2:]:
        load.start()
    top = me + reach >= devices

    def enter():
        pl.semaphore_wait(barrier, peers - below)

    @pl.when(top)
    def _():
        enter()
        for q in range(reach):
            to = me + q + 1

            @pl.when(to >= devices)
            def _():
                pl.semaphore_signal(
                    top_sem.at[q], inc=1, device_id=(wrap(to, devices),), device_id_type=MESH
                )

    loads[0].wait()

    row = lax.broadcasted_iota(jnp.int32, (32, 128), 0).astype(jnp.int16)
    one, zero = jnp.ones((32, 128), bf16), jnp.zeros((32, 128), bf16)

    def match(table, count, width, dest, height):
        for j in range(count):

            def build(b, carry):
                index = jnp.broadcast_to(table[j : j + 1, lanes(b, 128)], (32, 128))
                index = index.astype(jnp.int16) - row
                cols = pl.ds(pl.multiple_of(j * width + b * 128, 128), 128)
                for r in range(0, height, 32):
                    hit = jnp.where(index == jnp.int16(r), one, zero)
                    dest[r : r + 32, cols] = hit.astype(dest.dtype)
                return carry

            lax.fori_loop(0, width // 128, build, 0)

    match(send_cells, peers, halo, send_hot, cells)

    loads[1].wait()

    def split_x(start, count):
        def step(i, carry):
            t = start // level_count + 2 * i
            high, low = split(jnp.concatenate([tracers[t], tracers[t + 1]], axis=0))
            base = 2 * start + 16 * i
            low_x[pl.ds(pl.multiple_of(base, 16), 16), :] = high
            low_x[pl.ds(pl.multiple_of(base + count, 16), 16), :] = low
            return carry

        lax.fori_loop(0, count // 16, step, 0)

    def copy_of(kind, c, p, to):
        src, dst = (value_out, value_in) if kind == 0 else (grad_out, grad_in)
        start, count = [(1 + kind) * v for v in parts[c]]
        return pltpu.make_async_remote_copy(
            src_ref=src.at[p, pl.ds(start, count)],
            dst_ref=dst.at[p, pl.ds(start, count)],
            send_sem=send_sem.at[kind],
            recv_sem=recv_sem.at[kind, c],
            device_id=(wrap(to, devices),),
            device_id_type=MESH,
        )

    def all_of(kind, start, count, c):
        src, dst = (value_out, value_in) if kind == 0 else (grad_out, grad_in)
        return pltpu.make_async_remote_copy(
            src_ref=src.at[:, pl.ds((1 + kind) * start, (1 + kind) * count)],
            dst_ref=dst.at[:, pl.ds((1 + kind) * start, (1 + kind) * count)],
            send_sem=send_sem.at[kind],
            recv_sem=recv_sem.at[kind, c],
            device_id=(wrap(me + 1, devices),),
            device_id_type=MESH,
        )

    def send(kind, c, wanted):
        for bit in range(2):
            for q in order:
                to = me + (q + 1) * (1 - 2 * bit)
                copy = copy_of(kind, c, 2 * q + bit, to)
                if wanted is None:
                    copy.start()
                else:
                    pl.when(wanted(to))(copy.start)

    def above_ground(to):
        return to >= 0

    def under_ground(to):
        return to < 0

    def pack(terms, dest, start, count):
        part = pick(terms[pl.ds(2 * start, 2 * count), :], send_hot[:, : peers * halo])
        part = part[:count] + part[count:]
        for p in range(peers):
            dest[p, pl.ds(start, count), :] = part[:, p * halo : (p + 1) * halo]

    def local(terms, dest, scale, first, last):
        def step(b, carry):
            cols = lanes(b, WIDTH)
            part = pick(terms[...], hot[:cells, cols])
            for start, count in parts:
                start, count = scale * start, scale * count
                s = 2 * start
                dest[start : start + count, cols] = (
                    part[s : s + count] + part[s + count : s + 2 * count]
                )
            return carry

        lax.fori_loop(first, last, step, 0)

    def remote(arrived, terms, dest, start, count):
        for p in range(peers):
            high, low = split(arrived[p, pl.ds(start, count), :])
            terms[:count, p * halo : (p + 1) * halo] = high
            terms[count : 2 * count, p * halo : (p + 1) * halo] = low

        def step(b, carry):
            cols = lanes(b, 2 * WIDTH)
            part = pick(terms[: 2 * count, :], hot[cells:ext, cols])
            dest[start : start + count, cols] += part[:count] + part[count:]
            return carry

        lax.fori_loop(0, 3 * cells // (2 * WIDTH), step, 0)

    def gradient(start, per):
        def step(i, carry):
            t = start // level_count + 2 * i
            r = start + 16 * i
            here = jnp.concatenate([tracers[t], tracers[t + 1]], axis=0)
            at = pl.ds(pl.multiple_of(r, 16), 16)
            delta = [beside[at, j * cells : (j + 1) * cells] - here for j in range(3)]
            for k in range(2):
                total = lsq[0, k : k + 1, :] * delta[0]
                total = total + lsq[1, k : k + 1, :] * delta[1]
                total = total + lsq[2, k : k + 1, :] * delta[2]
                grads[k, at, :] = total
                high, low = split(total)
                base = 4 * start + k * per + 16 * i
                low_g[pl.ds(pl.multiple_of(base, 16), 16), :] = high
                low_g[pl.ds(pl.multiple_of(base + 2 * per, 16), 16), :] = low
            return carry

        lax.fori_loop(0, per // 16, step, 0)

    def finish(start, per):
        def step(i, carry):
            t = start // level_count + i
            at = pl.ds(pl.multiple_of(t * level_count, 8), level_count)
            f0 = pl.ds(pl.multiple_of(2 * start + i * level_count, 8), level_count)
            f1 = pl.ds(pl.multiple_of(2 * start + per + i * level_count, 8), level_count)
            for b in range(cells // 256):
                own = slice(b * 256, (b + 1) * 256)
                here = tracers[t, :, own]
                g0, g1 = grads[0, at, own], grads[1, at, own]
                outflow = None
                for j in range(3):
                    cols = slice(j * cells + b * 256, j * cells + (b + 1) * 256)
                    there = beside[at, cols]
                    own_face = here + g0 * own_off[0, j, :, own] + g1 * own_off[1, j, :, own]
                    far_face = (
                        there
                        + far[f0, cols] * far_off[0, j, :, own]
                        + far[f1, cols] * far_off[1, j, :, own]
                    )
                    side = flux[j, :, own]
                    face = jnp.where(side > 0, own_face, far_face)
                    face = jnp.maximum(face, jnp.minimum(here, there))
                    face = jnp.minimum(face, jnp.maximum(here, there))
                    term = side * face
                    outflow = term if outflow is None else outflow + term
                out[t, :, own] = here - inv_mass[:, own] * outflow
            return carry

        lax.fori_loop(0, per // level_count, step, 0)

    count_parts = len(parts)
    def pack_x(first, last):
        start, stop = parts[first][0], sum(parts[last])
        for part in parts[first : last + 1]:
            split_x(*part)
        whole = pick(low_x[2 * start : 2 * stop, :], send_hot[:, : peers * halo])
        for begin, count in parts[first : last + 1]:
            at = 2 * (begin - start)
            part = whole[at : at + count] + whole[at + count : at + 2 * count]
            for p in range(peers):
                value_out[p, begin : begin + count, :] = part[:, p * halo : (p + 1) * halo]

    pack_x(0, 0)
    interior = jnp.logical_not(jnp.logical_or(top, below > 0))
    pl.when(interior)(enter)

    @pl.when(below == 0)
    def _():
        send(0, 0, above_ground)

    late.wait()
    pack_x(1, count_parts - 1)

    @pl.when(below > 0)
    def _():
        enter()
        send(0, 0, above_ground)

    for c in range(1, count_parts):
        send(0, c, above_ground)
    loads[2].wait()
    match(near, 3, cells, hot, ext)
    loads[3].wait()
    local(low_x, beside, 1, 0, 1)

    @pl.when(below > 0)
    def _():
        for q in order[::-1]:
            to = me - q - 1

            @pl.when(to < 0)
            def _():
                pl.semaphore_wait(top_sem.at[q], 1)
                copy_of(0, 0, 2 * q + 1, to).start()

        for c in range(1, count_parts):
            send(0, c, under_ground)

    local(low_x, beside, 1, 1, 3 * cells // WIDTH)
    for c in range(count_parts):
        start, count = parts[c]
        all_of(0, start, count, c).wait_recv()
        remote(value_in, halo_x, beside, start, count)
        gradient(start, count)
        pack(low_g, grad_out, 2 * start, 2 * count)
        send(1, c, None)
    local(low_g, far, 2, 0, 3 * cells // WIDTH)
    for load in loads[4:]:
        load.wait()
    for c in range(count_parts):
        start, count = parts[c]
        all_of(1, start, count, c).wait_recv()
        remote(grad_in, halo_g, far, 2 * start, 2 * count)
        finish(start, count)
    for kind in range(2):
        all_of(kind, 0, rows, 0).wait_send()


def on_device(tracers, flux, lsq, own_off, far_off, inv_mass, near, send_cells):
    tracer_count, level_count, cells = tracers.shape
    rows = tracer_count * level_count
    peers, halo = send_cells.shape
    sizes = PARTS if 16 * sum(PARTS) == rows else (rows // 16,)
    parts, start = [], 0
    for size in sizes:
        parts.append((start, 16 * size))
        start += 16 * size
    per = 16 * max(sizes)
    lsq = lsq.transpose(1, 0, 2)
    operands = (tracers, flux, lsq, own_off, far_off, inv_mass, near, send_cells)
    ext = cells + peers * halo
    f32, bf16 = jnp.float32, jnp.bfloat16
    return pl.pallas_call(
        functools.partial(kernel, parts),
        out_shape=jax.ShapeDtypeStruct(tracers.shape, f32),
        in_specs=[pl.BlockSpec(memory_space=pltpu.HBM)] * 8,
        out_specs=pl.BlockSpec(memory_space=pltpu.VMEM),
        scratch_shapes=[pltpu.VMEM(a.shape, a.dtype) for a in operands]
        + [
            pltpu.SemaphoreType.DMA((9,)),
            pltpu.VMEM((ext, 3 * cells + 128), ONE_HOT),
            pltpu.VMEM((cells, peers * halo + 128), ONE_HOT),
            pltpu.VMEM((2 * rows, cells), bf16),
            pltpu.VMEM((4 * rows, cells), bf16),
            pltpu.VMEM((2, rows, cells), f32),
            pltpu.VMEM((rows, 3 * cells), f32),
            pltpu.VMEM((2 * rows, 3 * cells), f32),
            pltpu.VMEM((peers, rows, halo), f32),
            pltpu.VMEM((peers, rows, halo), f32),
            pltpu.VMEM((peers, 2 * rows, halo), f32),
            pltpu.VMEM((peers, 2 * rows, halo), f32),
            pltpu.VMEM((2 * per, peers * halo), bf16),
            pltpu.VMEM((4 * per, peers * halo), bf16),
            pltpu.SemaphoreType.DMA((2,)),
            pltpu.SemaphoreType.DMA((2, len(parts))),
            pltpu.SemaphoreType.REGULAR((peers // 2,)),
        ],
        compiler_params=pltpu.CompilerParams(
            collective_id=0, has_side_effects=True, vmem_limit_bytes=40 * 1024 * 1024
        ),
        name="step",
    )(*[pltpu.with_memory_space_constraint(a, pltpu.HBM) for a in operands])


def solution(mesh):
    placed = (
        P(None, None, "dom"),
        P(None, None, "dom"),
        P(None, None, "dom"),
        P(None, None, None, "dom"),
        P(None, None, None, "dom"),
        P(None, "dom"),
        P(None, "dom"),
        P(None, "dom"),
    )
    return jax.shard_map(
        on_device, mesh=mesh, in_specs=placed, out_specs=P(None, None, "dom"), check_vma=False
    )
```
